128 devices in a mesh: row: 8 (over y_lo, z), col: 16 (over x, y_hi, core).
Axes of the slice: x: 4, y: 4 (y_hi: 2, y_lo: 2; y = y_hi * 2 + y_lo), z: 4, core: 2. Of those that a mesh axis runs over, the one named last changes fastest.
Arguments:
- tokens: bfloat16 [12288, 8192], P(('row', 'col')), may hold values from -6 to 6
- up_weight: bfloat16 [8192, 14336], P('row', 'col'), may hold values from -0.0625 to 0.0625
Outputs:
- projected: bfloat16 [12288, 14336], P('row', 'col')
The draws below stay inside these ranges and needn't reach their ends.
All inputs are finite; a program needn't handle non-finite values.
Results may differ from the reference program's by a relative error of at most 0.001.
Values may be sent and summed in bfloat16 or wider, within the bound.
No kernel may reach another device: no remote copies, remote signals or barrier semaphores. Data moves between devices by JAX's collectives and lax.ppermute only.
A program may use at most 128 MiB of HBM per device.

```python
import jax
import jax.numpy as jnp

D = 8192
FF = 14336
TOKENS = 12288


def block_levels(stream_key, shape, pieces, least, high):
    gain = 1.0
    for axis_at, blocks in pieces:
        heights = jax.random.uniform(jax.random.fold_in(jax.random.fold_in(stream_key, 6), axis_at), (blocks,), jnp.float32, least / len(pieces), high / len(pieces))
        gain = gain * jnp.repeat(jnp.exp(heights), shape[axis_at] // blocks).reshape((-1,) + (1,) * (len(shape) - 1 - axis_at))
    return gain


def scatter_about(stream_key, extent, scale, bound, pieces=(), held_as=jnp.bfloat16):
    array = jax.random.normal(stream_key, extent, jnp.float32) * scale
    if len(pieces) > 0:
        array = block_levels(stream_key, extent, pieces, -0.22, 0.18) * array
    return jnp.clip(array, min=-bound, max=bound).astype(held_as)


def setup_inputs(seed: int = 0) -> dict:
    arg_keys = jax.random.split(jax.random.key(seed), 3)
    return {
        "tokens": scatter_about(arg_keys[0], (TOKENS, D), 1.0, 6.0, ((0, 128),)),
        "up_weight": scatter_about(arg_keys[1], (D, FF), D ** -0.5, 0.0625, ((0, 8), (1, 16))),
    }


def reference(tokens, up_weight):
    sums = jnp.dot(tokens.astype(jnp.float32), up_weight.astype(jnp.float32), preferred_element_type=jnp.float32)
    return sums.astype(jnp.bfloat16)
```

```python
import functools

import jax
import jax.numpy as jnp
from jax import lax
from jax.experimental import pallas as pl
from jax.experimental.pallas import tpu as pltpu
from jax.sharding import PartitionSpec as P

N = 896
KB = 1024
ROWS = 96


def row_perm(fn):
    return [(yl * 4 + z, fn(yl, z)[0] * 4 + fn(yl, z)[1]) for yl in range(2) for z in range(4)]


def col_perm(fn):
    at = lambda x, yh, c: x * 4 + yh * 2 + c
    return [(at(x, yh, c), at(*fn(x, yh, c))) for x in range(4) for yh in range(2) for c in range(2)]


WAYS = {
    "z+": ("row", row_perm(lambda yl, z: (yl, (z + 1) % 4))),
    "z-": ("row", row_perm(lambda yl, z: (yl, (z + 3) % 4))),
    "yl": ("row", row_perm(lambda yl, z: (1 - yl, z))),
    "x+": ("col", col_perm(lambda x, yh, c: ((x + 1) % 4, yh, c))),
    "x-": ("col", col_perm(lambda x, yh, c: ((x + 3) % 4, yh, c))),
    "yh": ("col", col_perm(lambda x, yh, c: (x, 1 - yh, c))),
    "co": ("col", col_perm(lambda x, yh, c: (x, yh, 1 - c))),
}

STEPS = [
    ("wLA", "z+", "wA"), ("wRB", "z-", "wB"), ("tL", "x+", "t"), ("tR", "x-", "t"), ("t1", "yh", "t"),
    ("wLB", "z+", "wB"), ("wRA", "z-", "wA"), ("w1A", "yl", "wA"), ("w1B", "yl", "wB"), ("ct", "co", "t"),
    ("wDA", "z+", "wLA"), ("wDB", "z-", "wRB"),
    ("tLA", "tL"), ("tDA", "x+", "tLA"), ("tRB", "tR"), ("tDB", "x-", "tRB"), ("t1L", "x+", "t1"), ("t1R", "x-", "t1"),
    ("ct1", "co", "t1"), ("ctL", "co", "tL"), ("ctR", "co", "tR"),
    ("w1LA", "z+", "w1A"), ("w1RA", "z-", "w1A"), ("ctDA", "co", "tDA"), ("ctDB", "co", "tDB"),
    ("k1",),
    ("w1LB", "z+", "w1B"), ("w1RB", "z-", "w1B"),
    ("w1DA", "z+", "w1LA"),
    ("t1LA", "t1L"), ("t1DA", "x+", "t1LA"), ("t1RB", "t1R"), ("t1DB", "x-", "t1RB"), ("ct1L", "co", "t1L"), ("ct1R", "co", "t1R"),
    ("k2",),
    ("w1DB", "z-", "w1RB"),
    ("k3",),
    ("ct1DA", "co", "t1DA"), ("ct1DB", "co", "t1DB"),
    ("k4",),
    ("k5",),
]
FAR = {"": 0, "L": 3, "R": 1, "D": 2}


def kernel(plan, at_ref, *refs):
    n_t, n_w, n_a = len(plan["t"]), len(plan["w"]), len(plan["acc"])
    t_refs, w_refs, a_refs = refs[:n_t], refs[n_t : n_t + n_w], refs[n_t + n_w : n_t + n_w + n_a]
    out_ref, t_vm, w_vm, acc, sem_t, sem_w, sem_a, *rest = refs[n_t + n_w + n_a :]
    blocks = plan["blocks"]
    a_copies = []
    for i, (first, rows) in enumerate(plan["acc"]):
        a_copies.append(pltpu.make_async_copy(a_refs[i], acc.at[pl.ds(first, rows)], sem_a.at[i]))
    copies = []
    for b, block in enumerate(blocks):
        col = pl.multiple_of(at_ref[plan["col"][b]], KB)
        mine = []
        for i, (name, row, rows) in enumerate(plan["t"]):
            if row >= block[0] and row < block[1]:
                mine.append(pltpu.make_async_copy(t_refs[i].at[:, pl.ds(col, KB)], t_vm.at[b, pl.ds(row, rows)], sem_t.at[b, i]))
        for i, (name, b_, row, rows) in enumerate(plan["w"]):
            if b_ == b:
                mine.append(pltpu.make_async_copy(w_refs[i], w_vm.at[b, pl.ds(row, rows)], sem_w.at[i]))
        copies.append(mine)
    for c in copies[0] + a_copies + sum(copies[1:], []):
        c.start()
    started = set(r for first, rows in plan["acc"] for r in range(first, first + rows, ROWS))
    for b, (lo, hi) in enumerate(blocks):
        for c in copies[b]:
            c.wait()
        if b == 0:
            for c in a_copies:
                c.wait()
        tile = plan["tile"]
        fresh = lo not in started
        started |= set(range(lo, hi, ROWS))

        @pl.loop(0, (hi - lo) // tile)
        def _(i, b=b, lo=lo, fresh=fresh):
            at = pl.ds(pl.multiple_of(lo + i * tile, 16), tile)
            part = jnp.dot(t_vm[b, at], w_vm[b], preferred_element_type=jnp.float32)
            acc[at] = part if fresh else acc[at] + part

    if not plan["last"]:
        c = pltpu.make_async_copy(acc, out_ref, sem_a.at[0])
        c.start()
        c.wait()
    else:
        res, sem_o = rest
        outs = []
        for i in range(16):
            at = pl.ds(i * ROWS, ROWS)
            res[at] = acc[at].astype(jnp.bfloat16)
            to = pl.multiple_of(at_ref[8 + i], 16)
            outs.append(pltpu.make_async_copy(res.at[at], out_ref.at[pl.ds(to, ROWS)], sem_o.at[i]))
            outs[-1].start()
        for c in outs:
            c.wait()


def call(at, got, accs, rows, t, w, blocks, acc=(), tile=256, last=False):
    t_in, w_in = [got[n] for n, _ in t], [got[n] for n, *_ in w]
    plan = {
        "t": [(n, r, v.shape[0]) for (n, r), v in zip(t, t_in)],
        "w": [(n, b, r, v.shape[0]) for (n, b, r), v in zip(w, w_in)],
        "acc": [(r, v.shape[0]) for r, v in zip(acc, accs)],
        "blocks": [b[1:] for b in blocks],
        "col": [b[0] for b in blocks],
        "tile": tile,
        "last": last,
    }
    nb = len(blocks)
    scratch = [
        pltpu.VMEM((nb, rows, KB), jnp.bfloat16),
        pltpu.VMEM((nb, KB, N), jnp.bfloat16),
        pltpu.VMEM((rows, N), jnp.float32),
        pltpu.SemaphoreType.DMA((nb, len(t))),
        pltpu.SemaphoreType.DMA((len(w),)),
        pltpu.SemaphoreType.DMA((max(1, len(accs)),)),
    ]
    if last:
        scratch += [pltpu.VMEM((rows, N), jnp.bfloat16), pltpu.SemaphoreType.DMA((16,))]
    flops = sum(2 * (hi - lo) * KB * N for _, lo, hi in blocks)
    hbm = pl.BlockSpec(memory_space=pltpu.HBM)
    return pl.pallas_call(
        functools.partial(kernel, plan),
        out_shape=jax.ShapeDtypeStruct((rows, N), jnp.bfloat16 if last else jnp.float32),
        in_specs=[pl.BlockSpec(memory_space=pltpu.SMEM)] + [hbm] * (len(t_in) + len(w_in) + len(accs)),
        out_specs=hbm,
        scratch_shapes=scratch,
        compiler_params=pltpu.CompilerParams(vmem_limit_bytes=50 * 2**20),
        cost_estimate=pl.CostEstimate(flops=flops, bytes_accessed=nb * rows * KB * 2, transcendentals=0),
    )(at, *t_in, *w_in, *accs)


def pieces(one, base):
    own = [(one + "", 0), (one + "L", 96), (one + "R", 192), (one + "DA", 288), (one + "DB", 336)]
    return [("t" + n, base + r) for n, r in own] + [("ct" + n, base + 384 + r) for n, r in own]


def on_device(tokens, up_weight):
    r, c = lax.axis_index("row"), lax.axis_index("col")
    yl, z = r // 4, r % 4
    x, yh, co = c // 4, c // 2 % 2, c % 2
    at = [((yl ^ one) * 4 + (z + FAR[k]) % 4) * KB for one in range(2) for k in ("", "L", "R", "D")]
    at += [
        ((x + FAR[k]) % 4 * 4 + (yh ^ one) * 2 + (co ^ cc)) * ROWS
        for one in range(2) for cc in range(2) for k in ("", "L", "R", "D")
    ]
    at = jnp.stack(at).astype(jnp.int32)
    got = {"t": tokens, "wA": up_weight[:512], "wB": up_weight[512:]}
    w0 = [("w" + k + h, b, 512 * (h == "B")) for b, k in enumerate(("", "L", "R", "D")) for h in "AB"]
    w1 = [("w1" + k + h, b, 512 * (h == "B")) for b, k in enumerate(("", "L", "R")) for h in "AB"]
    for step in STEPS:
        if len(step) == 3:
            name, way, operand = step
            got[name] = lax.ppermute(got[operand], *WAYS[way])
            continue
        if len(step) == 2:
            whole, half = got[step[1]], ROWS // 2
            got[step[0]] = whole[:half] if step[0][-1] == "A" else whole[half:]
            continue
        name, = step
        if name == "k1":
            a0 = call(at, got, [], 768, pieces("", 0), w0, [(b, 0, 768) for b in range(4)])
        if name == "k2":
            t = [("t1", 0), ("t1L", 96), ("t1R", 192), ("ct1", 288), ("ct1L", 384), ("ct1R", 480)]
            a1 = call(at, got, [], 576, t, w0, [(b, 0, 576) for b in range(4)], tile=288)
        if name == "k3":
            a0 = call(at, got, [a0], 768, pieces("", 0), w1, [(b, 0, 768) for b in (4, 5, 6)], acc=(0,))
        if name == "k4":
            t = [("t1", 0), ("t1L", 96), ("t1R", 192), ("ct1", 288), ("ct1L", 384), ("ct1R", 480)]
            t += [("t1DA", 576), ("t1DB", 624), ("ct1DA", 672), ("ct1DB", 720)]
            w = [(n, b, r_) for n, b, r_ in w0] + [(n, b + 4, r_) for n, b, r_ in w1]
            a1 = call(
                at, got, [a1], 768, t, w,
                [(b, 576, 768) for b in range(4)] + [(b, 0, 768) for b in (4, 5, 6)], acc=(0,), tile=192,
            )
        if name == "k5":
            t = pieces("", 0) + [("t1", 768), ("t1L", 864), ("t1R", 960), ("ct1", 1056), ("ct1L", 1152), ("ct1R", 1248)]
            t += [("t1DA", 1344), ("t1DB", 1392), ("ct1DA", 1440), ("ct1DB", 1488)]
            order = list(range(8)) + [8, 9, 10, 12, 13, 14, 11, 15]
            at5 = jnp.concatenate([at[:8], jnp.stack([at[8 + o] for o in order])])
            return call(
                at5, got, [a0, a1], 1536, t, [("w1DA", 0, 0), ("w1DB", 0, 512)], [(7, 0, 1536)],
                acc=(0, 768), last=True,
            )


def solution(mesh):
    return jax.shard_map(
        on_device, mesh=mesh, in_specs=(P(("row", "col"), None), P("row", "col")), out_specs=P("row", "col"), check_vma=False
    )
```

```python
import functools

import jax
import jax.numpy as jnp
from jax import lax
from jax.experimental import pallas as pl
from jax.experimental.pallas import tpu as pltpu
from jax.sharding import PartitionSpec as P

N = 896
KB = 1024
ROWS = 96


def row_perm(fn):
    return [(yl * 4 + z, fn(yl, z)[0] * 4 + fn(yl, z)[1]) for yl in range(2) for z in range(4)]


def col_perm(fn):
    at = lambda x, yh, c: x * 4 + yh * 2 + c
    return [(at(x, yh, c), at(*fn(x, yh, c))) for x in range(4) for yh in range(2) for c in range(2)]


WAYS = {
    "z+": ("row", row_perm(lambda yl, z: (yl, (z + 1) % 4))),
    "z-": ("row", row_perm(lambda yl, z: (yl, (z + 3) % 4))),
    "yl": ("row", row_perm(lambda yl, z: (1 - yl, z))),
    "x+": ("col", col_perm(lambda x, yh, c: ((x + 1) % 4, yh, c))),
    "x-": ("col", col_perm(lambda x, yh, c: ((x + 3) % 4, yh, c))),
    "yh": ("col", col_perm(lambda x, yh, c: (x, 1 - yh, c))),
    "co": ("col", col_perm(lambda x, yh, c: (x, yh, 1 - c))),
}

STEPS = [
    ("wLA", "z+", "wA"), ("wRB", "z-", "wB"), ("tLA", "x+", "tA"), ("tRB", "x-", "tB"), ("w1A", "yl", "wA"),
    ("wLB", "z+", "wB"), ("wRA", "z-", "wA"), ("tLB", "x+", "tB"), ("tRA", "x-", "tA"),
    ("t1A", "yh", "tA"), ("w1B", "yl", "wB"), ("t1B", "yh", "tB"), ("ct", "co", "t"),
    ("tDA", "x+", "tLA"), ("tDB", "x-", "tRB"), ("wDA", "z+", "wLA"), ("wDB", "z-", "wRB"),
    ("ctLA", "co", "tLA"), ("ctRB", "co", "tRB"),
    ("w1LA", "z+", "w1A"), ("ctLB", "co", "tLB"), ("ctRA", "co", "tRA"),
    ("t1LA", "x+", "t1A"), ("t1RA", "x-", "t1A"), ("ct1A", "co", "t1A"),
    ("kA",),
    ("ctDA", "co", "tDA"), ("ctDB", "co", "tDB"),
    ("w1RB", "z-", "w1B"), ("w1LB", "z+", "w1B"), ("w1RA", "z-", "w1A"),
    ("kB",),
    ("t1RB", "x-", "t1B"), ("t1LB", "x+", "t1B"), ("t1DA", "x+", "t1LA"),
    ("ct1B", "co", "t1B"), ("ct1LA", "co", "t1LA"), ("ct1RA", "co", "t1RA"),
    ("w1DA", "z+", "w1LA"), ("w1DB", "z-", "w1RB"),
    ("t1DB", "x-", "t1RB"), ("ct1RB", "co", "t1RB"), ("ct1LB", "co", "t1LB"),
    ("kC",),
    ("kD",),
    ("ct1DA", "co", "t1DA"), ("ct1DB", "co", "t1DB"),
    ("kE",),
    ("kF",),
]
FAR = {"": 0, "L": 3, "R": 1, "D": 2}


def rows_of(names):
    return [
        (p, ROWS * i + r) for i, n in enumerate(names) for p, r in ([(n, 0)] if n in ("t", "ct") else [(n + "A", 0), (n + "B", 48)])
    ]


A = ["t", "tL", "tR", "ct", "ctL", "ctR"]
D0 = ["tD", "ctD"]
B1 = ["t1", "t1L", "t1R", "ct1", "ct1L", "ct1R"]
B2 = ["t1D", "ct1D"]

W = [(b, 0, KB, [(f"w{k}A", 0, 512), (f"w{k}B", 0, 512)]) for b, k in enumerate(("", "L", "R", "D", "1", "1L", "1R", "1D"))]

KERNELS = {
    "kA": (A, [], [(0, 576, W[:3])]),
    "kB": (A + D0, [("kA", 0)], [(0, 576, W[3:5]), (576, 768, W[:5])]),
    "kC": (B1, [], [(0, 576, W[:5])]),
    "kD": (A + D0 + B1, [("kB", 0), ("kC", 768)], [(0, 1344, W[5:7])]),
    "kE": (B2, [], [(0, 192, W[:7])]),
    "kF": (A + D0 + B1 + B2, [("kD", 0), ("kE", 1344)], [(0, 1536, W[7:])]),
}
TILE = 288
VMEM, LAST_VMEM = 5, 7


def kernel(plan, *refs):
    r, c = lax.axis_index("row"), lax.axis_index("col")
    yl, z, x, yh, core = r // 4, r % 4, c // 4, c // 2 % 2, c % 2
    block_at = [((yl ^ one) * 4 + (z + FAR[k]) % 4) * KB for one in range(2) for k in ("", "L", "R", "D")]
    n_t, n_w, n_a = len(plan["t"]), len(plan["w"]), len(plan["acc"])
    t_refs, w_refs, a_refs = refs[:n_t], refs[n_t : n_t + n_w], refs[n_t + n_w : n_t + n_w + n_a]
    out_ref, *rest = refs[n_t + n_w + n_a :]
    rows_all = plan["rows"]

    def product(r, e, piece):
        block, k0, _, arrays = piece
        total, k = None, k0
        for name, first, rows in arrays:
            cols = pl.ds(pl.multiple_of(block_at[block] + k, 128), rows)
            lhs = [t_refs[i][:, cols] for i, (row, n) in enumerate(plan["t"]) if r <= row < e]
            lhs = lhs[0] if len(lhs) == 1 else jnp.concatenate(lhs, axis=0)
            part = jnp.dot(lhs, w_refs[plan["w"].index(name)][pl.ds(first, rows), :], preferred_element_type=jnp.float32)
            total = part if total is None else total + part
            k += rows
        return total

    tiles, have = [], {}
    for i, (first, rows) in enumerate(plan["acc"]):
        for r in range(first, first + rows, ROWS):
            have[r] = (i, r - first)
    done = set()
    for lo, hi, pieces in plan["groups"]:
        r = lo
        while r < hi:
            e, of = r, have.get(r)
            while e < hi and e - r < plan["tile"] and (e in done) == (r in done) and (
                e in done or (None if have.get(e) is None else have[e][0]) == (None if of is None else of[0])
            ):
                e += ROWS
            total = None
            for piece in pieces:
                part = product(r, e, piece)
                total = part if total is None else total + part
            at = pl.ds(r, e - r)
            if r in done:
                total = total + out_ref[at]
            elif of is not None:
                total = total + a_refs[of[0]][pl.ds(of[1], e - r)]
            if plan["last"]:
                res, sem_o = rest
                res[at] = total.astype(jnp.bfloat16)
                for q in range(r, e, ROWS):
                    name = plan["names"][q // ROWS]
                    far = (x + FAR[name.lstrip("ct1")]) % 4 * 4 + (yh ^ ("1" in name)) * 2 + (core ^ ("c" in name))
                    to = pl.multiple_of(far * ROWS, 16)
                    tiles.append(pltpu.make_async_copy(res.at[pl.ds(q, ROWS)], out_ref.at[pl.ds(to, ROWS)], sem_o.at[q // ROWS]))
                    tiles[-1].start()
            else:
                out_ref[at] = total
            done |= set(range(r, e, ROWS))
            r = e
    for c in tiles:
        c.wait()
    for r in range(0, rows_all, ROWS):
        if r not in done:
            i, first = have[r]
            out_ref[pl.ds(r, ROWS)] = a_refs[i][pl.ds(first, ROWS)]


def call(name, got, sums):
    names, taken, groups = KERNELS[name]
    rows, last = ROWS * len(names), name == "kF"
    layout = rows_of(names)
    arrays = []
    for _, _, pieces in groups:
        for piece in pieces:
            arrays += [a for a, _, _ in piece[3] if a not in arrays]
    t_in, w_in, a_in = [got[n] for n, _ in layout], [got[n] for n in arrays], [sums[k] for k, _ in taken]
    plan = {
        "rows": rows,
        "names": names,
        "t": [(r, v.shape[0]) for (_, r), v in zip(layout, t_in)],
        "w": arrays,
        "acc": [(first, v.shape[0]) for (_, first), v in zip(taken, a_in)],
        "groups": groups,
        "tile": TILE,
        "last": last,
    }
    width = [sum(p[2] for p in pieces) for _, _, pieces in groups]
    scratch = []
    if last:
        scratch += [pltpu.VMEM((rows, N), jnp.bfloat16), pltpu.SemaphoreType.DMA((16,))]
    flops = sum(2 * (hi - lo) * k * N for (lo, hi, _), k in zip(groups, width))
    vmem = pl.BlockSpec(memory_space=pltpu.VMEM)
    ins = [pltpu.with_memory_space_constraint(v, pltpu.MemorySpace.VMEM) for v in (*t_in, *w_in, *a_in)]
    return pl.pallas_call(
        functools.partial(kernel, plan),
        out_shape=jax.ShapeDtypeStruct((rows, N), jnp.bfloat16) if last else pltpu.MemorySpace.VMEM((rows, N), jnp.float32),
        in_specs=[vmem] * len(ins),
        out_specs=pl.BlockSpec(memory_space=pltpu.HBM) if last else vmem,
        scratch_shapes=scratch,
        compiler_params=pltpu.CompilerParams(vmem_limit_bytes=(LAST_VMEM if last else VMEM) * 2**20),
        cost_estimate=pl.CostEstimate(flops=flops, bytes_accessed=rows * sum(width) * 2, transcendentals=0),
    )(*ins)


def on_device(tokens, up_weight):
    got = {"t": tokens, "tA": tokens[:48], "tB": tokens[48:], "wA": up_weight[:512], "wB": up_weight[512:]}
    sums = {}
    for step in STEPS:
        if len(step) == 3:
            got[step[0]] = lax.ppermute(got[step[2]], *WAYS[step[1]])
        else:
            sums[step[0]] = call(step[0], got, sums)
    return sums["kF"]


def solution(mesh):
    return jax.shard_map(
        on_device, mesh=mesh, in_specs=(P(("row", "col"), None), P("row", "col")), out_specs=P("row", "col"), check_vma=False
    )
```

```python
import functools
import itertools

import jax
import jax.numpy as jnp
from jax import lax
from jax.experimental import pallas as pl
from jax.experimental.pallas import tpu as pltpu
from jax.sharding import PartitionSpec as P

N = 896
KB = 1024
ROWS = 96


F = 256
H = (KB - F) // 2


def way(fn):
    at = lambda yl, z, x, yh, c: (yl * 4 + z % 4) * 16 + x % 4 * 4 + yh * 2 + c
    places = itertools.product(range(2), range(4), range(4), range(2), range(2))
    return [(at(*p), at(*fn(*p))) for p in places]


WAYS = {
    "zP": way(lambda yl, z, x, yh, c: (yl, z + 1 - 2 * c, x, yh, c)),
    "zM": way(lambda yl, z, x, yh, c: (yl, z - 1 + 2 * c, x, yh, c)),
    "xP": way(lambda yl, z, x, yh, c: (yl, z, x + 1 - 2 * c, yh, c)),
    "xM": way(lambda yl, z, x, yh, c: (yl, z, x - 1 + 2 * c, yh, c)),
    "yl": way(lambda yl, z, x, yh, c: (1 - yl, z, x, yh, c)),
    "yh": way(lambda yl, z, x, yh, c: (yl, z, x, 1 - yh, c)),
    "co": way(lambda yl, z, x, yh, c: (yl, z, x, yh, 1 - c)),
}

STEPS = [
    ("t1", "yh", "t"), ("tP", "xP", "t"), ("tM", "xM", "t"),
    ("FP", "zP", "F"), ("FM", "zM", "F"), ("SP", "zP", "S"), ("SM", "zM", "S"), ("ct", "co", "t"),
    ("FD", "zP", "FP"),
    ("S1a", "yl", "Sa"), ("S1b", "yl", "Sb"),
    ("t1P", "xP", "t1"), ("t1M", "xM", "t1"), ("ct1", "co", "t1"), ("ctP", "co", "tP"), ("ctM", "co", "tM"), ("tD", "xP", "tP"),
    ("SD", "zP", "SP"),
    ("kA",),
    ("F1", "yl", "F"), ("F1P", "yl", "FP"), ("F1M", "yl", "FM"),
    ("S1aP", "zP", "S1a"), ("S1aM", "zM", "S1a"), ("F1D", "yl", "FD"),
    ("S1bP", "zP", "S1b"), ("S1bM", "zM", "S1b"),
    ("kB",),
    ("t1D", "xP", "t1P"), ("ct1P", "co", "t1P"), ("ct1M", "co", "t1M"),
    ("kC",),
    ("S1aD", "zP", "S1aP"),
    ("ctD", "co", "tD"),
    ("kD",),
    ("S1bD", "zP", "S1bP"),
    ("kE",),
    ("ct1D", "co", "t1D"),
    ("kF",),
    ("kG",),
]
A = ["t", "tP", "tM", "t1", "ct", "ctP", "ctM", "ct1"]
B1 = ["t1P", "t1M", "ct1P", "ct1M"]
D0 = ["tD", "ctD"]
B2 = ["t1D", "ct1D"]

W0 = [(b, 0, [(f"F{k}", F), (f"S{k}", KB - F)]) for b, k in enumerate(("", "P", "M"))]
WD = [(3, 0, [("FD", F), ("SD", KB - F)])]
S1 = [(4, F, [("S1a", H), ("S1b", H)])]
W1 = [(4, 0, [("F1", F)])] + [(b, 0, [(f"F1{k}", F), (f"S1a{k}", H), (f"S1b{k}", H)]) for b, k in ((5, "P"), (6, "M"))]
W1D = [(7, 0, [("F1D", F), ("S1aD", H), ("S1bD", H)])]

KERNELS = {
    "kA": (A, [], [(0, 768, W0)]),
    "kB": (A, [("kA", 0)], [(0, 768, WD + S1)]),
    "kC": (B1, [], [(0, 384, W0 + WD + S1)]),
    "kD": (D0, [], [(0, 192, W0 + WD + S1)]),
    "kE": (A + B1 + D0, [("kB", 0), ("kC", 768), ("kD", 1152)], [(0, 1344, W1)]),
    "kF": (A + B1 + D0, [("kE", 0)], [(0, 1344, W1D)]),
    "kG": (B2, [], [(0, 192, W0 + WD + S1 + W1 + W1D)]),
}
TILE = 384
VMEM, LAST_VMEM = 6, 8


def kernel(plan, *refs):
    row, col = lax.axis_index("row"), lax.axis_index("col")
    yl, z, x, yh, core = row // 4, row % 4, col // 4, col // 2 % 2, col % 2
    far = lambda name, c: 3 - 2 * c if "P" in name else 1 + 2 * c if "M" in name else 2 if "D" in name else 0
    block_at = [((yl ^ one) * 4 + (z + far(k, core)) % 4) * KB for one in range(2) for k in ("", "P", "M", "D")]
    n_t, n_w, n_a = len(plan["t"]), len(plan["w"]), len(plan["acc"])
    t_refs, w_refs, a_refs = refs[:n_t], refs[n_t : n_t + n_w], refs[n_t + n_w : n_t + n_w + n_a]
    out_ref, *rest = refs[n_t + n_w + n_a + plan["onto"] :]

    def product(r, e, piece):
        block, k, arrays = piece
        total = None
        for name, rows in arrays:
            cols = pl.ds(pl.multiple_of(block_at[block] + k, 128), rows)
            lhs = jnp.concatenate([t_refs[i][:, cols] for i in range(r // ROWS, e // ROWS)], axis=0)
            part = jnp.dot(lhs, w_refs[plan["w"].index(name)][...], preferred_element_type=jnp.float32)
            total = part if total is None else total + part
            k += rows
        return total

    tiles, have = [], {}
    for i, (first, rows) in enumerate(plan["acc"]):
        for r in range(first, first + rows, ROWS):
            have[r] = (i, r - first)
    done = set()
    for lo, hi, pieces in plan["groups"]:
        r = lo
        while r < hi:
            e, of = r, have.get(r)
            while e < hi and e - r < plan["tile"] and (e in done) == (r in done) and (
                e in done or (None if have.get(e) is None else have[e][0]) == (None if of is None else of[0])
            ):
                e += ROWS
            total = None
            for piece in pieces:
                part = product(r, e, piece)
                total = part if total is None else total + part
            at = pl.ds(r, e - r)
            if r in done:
                total = total + out_ref[at]
            elif of is not None:
                total = total + a_refs[of[0]][pl.ds(of[1], e - r)]
            if plan["last"]:
                res, sem_o = rest
                res[at] = total.astype(jnp.bfloat16)
                for q in range(r, e, ROWS):
                    name = plan["names"][q // ROWS]
                    c = core ^ ("c" in name)
                    place = (x + far(name, c)) % 4 * 4 + (yh ^ ("1" in name)) * 2 + c
                    to = pl.multiple_of(place * ROWS, 16)
                    tiles.append(pltpu.make_async_copy(res.at[pl.ds(q, ROWS)], out_ref.at[pl.ds(to, ROWS)], sem_o.at[q // ROWS]))
                    tiles[-1].start()
            else:
                out_ref[at] = total
            done |= set(range(r, e, ROWS))
            r = e
    for c in tiles:
        c.wait()


def call(name, got, sums):
    names, taken, groups = KERNELS[name]
    rows, last, onto = ROWS * len(names), name in ("kF", "kG"), name == "kG"
    arrays = []
    for _, _, blocks in groups:
        for block in blocks:
            arrays += [a for a, _ in block[2] if a not in arrays]
    t_in, w_in, a_in = [got[n] for n in names], [got[n] for n in arrays], [sums[k] for k, _ in taken]
    plan = {
        "names": names,
        "t": names,
        "w": arrays,
        "acc": [(first, v.shape[0]) for (_, first), v in zip(taken, a_in)],
        "groups": groups,
        "tile": TILE,
        "last": last,
        "onto": int(onto),
    }
    width = [sum(rows for b in blocks for _, rows in b[2]) for _, _, blocks in groups]
    scratch = []
    if last:
        scratch += [pltpu.VMEM((rows, N), jnp.bfloat16), pltpu.SemaphoreType.DMA((len(names),))]
    flops = sum(2 * (hi - lo) * k * N for (lo, hi, _), k in zip(groups, width))
    vmem = pl.BlockSpec(memory_space=pltpu.VMEM)
    ins = [pltpu.with_memory_space_constraint(v, pltpu.MemorySpace.VMEM) for v in (*t_in, *w_in, *a_in)]
    n_in, hbm = len(ins), pl.BlockSpec(memory_space=pltpu.HBM)
    return pl.pallas_call(
        functools.partial(kernel, plan),
        out_shape=jax.ShapeDtypeStruct((16 * ROWS, N), jnp.bfloat16) if last else pltpu.MemorySpace.VMEM((rows, N), jnp.float32),
        in_specs=[vmem] * n_in + [hbm] * onto,
        out_specs=hbm if last else vmem,
        input_output_aliases={n_in: 0} if onto else {},
        scratch_shapes=scratch,
        compiler_params=pltpu.CompilerParams(vmem_limit_bytes=(LAST_VMEM if last else VMEM) * 2**20),
        cost_estimate=pl.CostEstimate(flops=flops, bytes_accessed=rows * sum(width) * 2, transcendentals=0),
    )(*ins, *([sums["kF"]] if onto else []))


def on_device(tokens, up_weight):
    got = {"t": tokens, "F": up_weight[:F], "S": up_weight[F:], "Sa": up_weight[F : F + H], "Sb": up_weight[F + H :]}
    sums = {}
    for step in STEPS:
        if len(step) == 3:
            got[step[0]] = lax.ppermute(got[step[2]], ("row", "col"), WAYS[step[1]])
        else:
            sums[step[0]] = call(step[0], got, sums)
    return sums["kG"]


def solution(mesh):
    return jax.shard_map(
        on_device, mesh=mesh, in_specs=(P(("row", "col"), None), P("row", "col")), out_specs=P("row", "col"), check_vma=False
    )
```

```python
import functools
import itertools

import jax
import jax.numpy as jnp
from jax import lax
from jax.experimental import pallas as pl
from jax.experimental.pallas import tpu as pltpu
from jax.sharding import PartitionSpec as P

N = 896
KB = 1024
ROWS = 96


F = 256
HA, HB = 512, 256


def way(fn):
    at = lambda yl, z, x, yh, c: (yl * 4 + z % 4) * 16 + x % 4 * 4 + yh * 2 + c
    places = itertools.product(range(2), range(4), range(4), range(2), range(2))
    return [(at(*p), at(*fn(*p))) for p in places]


WAYS = {
    "zP": way(lambda yl, z, x, yh, c: (yl, z + 1 - 2 * c, x, yh, c)),
    "zM": way(lambda yl, z, x, yh, c: (yl, z - 1 + 2 * c, x, yh, c)),
    "xP": way(lambda yl, z, x, yh, c: (yl, z, x + 1 - 2 * c, yh, c)),
    "xM": way(lambda yl, z, x, yh, c: (yl, z, x - 1 + 2 * c, yh, c)),
    "yl": way(lambda yl, z, x, yh, c: (1 - yl, z, x, yh, c)),
    "yh": way(lambda yl, z, x, yh, c: (yl, z, x, 1 - yh, c)),
    "co": way(lambda yl, z, x, yh, c: (yl, z, x, yh, 1 - c)),
}

STEPS = [
    ("t1", "yh", "t"), ("FP", "zP", "F"), ("FM", "zM", "F"), ("tP", "xP", "t"), ("tM", "xM", "t"),
    ("SP", "zP", "S"), ("SM", "zM", "S"), ("ct", "co", "t"),
    ("FD", "zP", "FP"),
    ("S1a", "yl", "Sa"), ("S1b", "yl", "Sb"),
    ("t1P", "xP", "t1"), ("t1M", "xM", "t1"), ("ct1", "co", "t1"), ("ctP", "co", "tP"), ("ctM", "co", "tM"), ("tD", "xP", "tP"),
    ("SD", "zP", "SP"),
    ("kA",),
    ("F1", "yl", "F"), ("F1P", "yl", "FP"), ("F1M", "yl", "FM"),
    ("S1aP", "zP", "S1a"), ("S1aM", "zM", "S1a"), ("F1D", "yl", "FD"),
    ("S1bP", "zP", "S1b"), ("S1bM", "zM", "S1b"),
    ("kB",),
    ("kS",),
    ("t1Da", "xP", "t1Pa"), ("t1Db", "xP", "t1Pb"), ("ct1P", "co", "t1P"), ("ct1M", "co", "t1M"),
    ("kC",),
    ("S1aD", "zP", "S1aP"),
    ("ctD", "co", "tD"),
    ("kD",),
    ("S1bD", "zP", "S1bP"),
    ("kE",),
    ("ct1Da", "co", "t1Da"),
    ("kI",),
    ("kK",),
    ("kJ",),
    ("ct1Db", "co", "t1Db"),
    ("kF",),
    ("kG",),
]
A = ["t", "tP", "tM", "t1", "ct", "ctP", "ctM", "ct1"]
B1 = ["t1P", "t1M", "ct1P", "ct1M"]
D0 = ["tD", "ctD"]
B2 = ["t1D", "ct1D"]

W0 = [(b, 0, [(f"F{k}", F), (f"S{k}", KB - F)]) for b, k in enumerate(("", "P", "M"))]
WD = [(3, 0, [("FD", F), ("SD", KB - F)])]
S1 = [(4, F, [("S1a", HA), ("S1b", HB)])]
W1 = [(4, 0, [("F1", F)]), (5, 0, [("F1P", F), ("S1aP", HA)]), (6, F, [("S1aM", HA)])]
W2 = [(5, F + HA, [("S1bP", HB)]), (6, 0, [("F1M", F)]), (6, F + HA, [("S1bM", HB)])]
W3, W4, W5 = [(7, F, [("S1aD", HA)])], [(7, 0, [("F1D", F)])], [(7, F + HA, [("S1bD", HB)])]

ALL = A + B1 + D0 + B2
B2_AT = ROWS * len(A + B1 + D0)


def piece_of(name, block):
    return name + "ab"[block // 4] if name in B2 else name


KERNELS = {
    "kA": [(0, 768, W0)],
    "kB": [(0, 768, WD + S1)],
    "kC": [(768, 1152, W0 + WD + S1)],
    "kD": [(0, 1152, W1)],
    "kE": [(1152, 1344, W0 + WD + S1 + W1)],
    "kI": [(0, 1344, W2)],
    "kJ": [(0, 1344, W3)],
    "kF": [(0, 1344, W4)],
    "kK": [(1344, 1536, W0 + WD)],
    "kG": [(0, 1344, W5), (1344, 1536, S1 + W1 + W2 + W3 + W4 + W5)],
}
TILE = 384
VMEM, LAST_VMEM = 2, 6


def sum_of(parts):
    return functools.reduce(lambda a, b: a + b, parts)


def kernel(plan, *refs):
    row, col = lax.axis_index("row"), lax.axis_index("col")
    yl, z, x, yh, core = row // 4, row % 4, col // 4, col // 2 % 2, col % 2
    far = lambda name, c: 3 - 2 * c if "P" in name else 1 + 2 * c if "M" in name else 2 if "D" in name else 0
    block_at = [((yl ^ one) * 4 + (z + far(k, core)) % 4) * KB for one in range(2) for k in ("", "P", "M", "D")]
    n_t, n_w = len(plan["t"]), len(plan["w"])
    t_refs, w_refs, refs = refs[:n_t], refs[n_t : n_t + n_w], refs[n_t + n_w :]
    sums_ref, refs = (refs[0], refs[1:]) if plan["taken"] else (None, refs)
    out_ref, *rest = refs

    def product(r, e, piece):
        block, k, arrays = piece
        total = None
        for name, rows in arrays:
            at = block_at[block] + k
            if r >= B2_AT:
                at = at - (yl ^ (block // 4)) * (4 * KB)
            cols = pl.ds(pl.multiple_of(at, 128), rows)
            lhs = [t_refs[plan["t"].index(piece_of(n, block))][:, cols] for n in ALL[r // ROWS : e // ROWS]]
            lhs = jnp.concatenate(lhs, axis=0)
            part = jnp.dot(lhs, w_refs[plan["w"].index(name)][...], preferred_element_type=jnp.float32)
            total = part if total is None else total + part
            k += rows
        return total

    started = []
    for lo, hi, blocks in plan["groups"]:
        for r in range(lo, hi, TILE):
            e = min(hi, r + TILE)
            at = pl.ds(r, e - r)
            total = sum_of([product(r, e, block) for block in blocks])
            if blocks[0] not in W0:
                total = total + sums_ref[at]
            if not plan["last"]:
                out_ref[at] = total
                continue
            res, sem = rest
            res[at] = total.astype(jnp.bfloat16)
            for q in range(r // ROWS, e // ROWS):
                c = core ^ ("c" in ALL[q])
                place = (x + far(ALL[q], c)) % 4 * 4 + (yh ^ ("1" in ALL[q])) * 2 + c
                to = out_ref.at[pl.ds(pl.multiple_of(place * ROWS, 16), ROWS)]
                started.append(pltpu.make_async_copy(res.at[pl.ds(q * ROWS, ROWS)], to, sem.at[q]))
                started[-1].start()
    for copy in started:
        copy.wait()


def call(name, got, sums):
    groups, last = KERNELS[name], name == "kG"
    names, arrays = [], []
    for lo, hi, blocks in groups:
        for n in ALL[lo // ROWS : hi // ROWS]:
            names += [p for p in dict.fromkeys(piece_of(n, b[0]) for b in blocks) if p not in names]
    for _, _, blocks in groups:
        for block in blocks:
            arrays += [a for a, _ in block[2] if a not in arrays]
    plan = {"t": names, "w": arrays, "taken": sums is not None, "groups": groups, "last": last}
    flops = sum(2 * (hi - lo) * rows * N for lo, hi, blocks in groups for b in blocks for _, rows in b[2])
    vmem = pl.BlockSpec(memory_space=pltpu.VMEM)
    ins = [got[n] for n in names + arrays] + ([] if sums is None else [sums])
    ins = [pltpu.with_memory_space_constraint(v, pltpu.MemorySpace.VMEM) for v in ins]
    shape = (len(ALL) * ROWS, N)
    return pl.pallas_call(
        functools.partial(kernel, plan),
        out_shape=jax.ShapeDtypeStruct(shape, jnp.bfloat16) if last else pltpu.MemorySpace.VMEM(shape, jnp.float32),
        in_specs=[vmem] * len(ins),
        out_specs=pl.BlockSpec(memory_space=pltpu.HBM) if last else vmem,
        input_output_aliases={} if last or sums is None else {len(ins) - 1: 0},
        scratch_shapes=[pltpu.VMEM(shape, jnp.bfloat16), pltpu.SemaphoreType.DMA((len(ALL),))] if last else [],
        compiler_params=pltpu.CompilerParams(vmem_limit_bytes=(LAST_VMEM if last else VMEM) * 2**20),
        cost_estimate=pl.CostEstimate(flops=flops, bytes_accessed=flops // 1000, transcendentals=0),
    )(*ins)


def halves(whole, own, other):
    yl = lax.axis_index("row") // 4
    own[...] = whole[:, pl.ds(pl.multiple_of(yl * (4 * KB), 4 * KB), 4 * KB)]
    other[...] = whole[:, pl.ds(pl.multiple_of((1 - yl) * (4 * KB), 4 * KB), 4 * KB)]


def cut(whole):
    vmem = pl.BlockSpec(memory_space=pltpu.VMEM)
    return pl.pallas_call(
        halves,
        out_shape=[pltpu.MemorySpace.VMEM((ROWS, 4 * KB), jnp.bfloat16)] * 2,
        in_specs=[vmem],
        out_specs=[vmem, vmem],
        compiler_params=pltpu.CompilerParams(vmem_limit_bytes=VMEM * 2**20),
        name="kS",
    )(pltpu.with_memory_space_constraint(whole, pltpu.MemorySpace.VMEM))


def on_device(tokens, up_weight):
    got = {"t": tokens, "F": up_weight[:F], "S": up_weight[F:], "Sa": up_weight[F : F + HA], "Sb": up_weight[F + HA :]}
    sums = None
    for step in STEPS:
        if len(step) == 3:
            got[step[0]] = lax.ppermute(got[step[2]], ("row", "col"), WAYS[step[1]])
        elif step == ("kS",):
            got["t1Pa"], got["t1Pb"] = cut(got["t1P"])
        else:
            sums = call(step[0], got, sums)
    return sums


def solution(mesh):
    return jax.shard_map(
        on_device, mesh=mesh, in_specs=(P(("row", "col"), None), P("row", "col")), out_specs=P("row", "col"), check_vma=False
    )
```

```python
import functools
import itertools

import jax
import jax.numpy as jnp
from jax import lax
from jax.experimental import pallas as pl
from jax.experimental.pallas import tpu as pltpu
from jax.sharding import PartitionSpec as P

N = 896
KB = 1024
ROWS = 96


F = 256
HA, HB = 512, 256


def way(fn):
    at = lambda yl, z, x, yh, c: (yl * 4 + z % 4) * 16 + x % 4 * 4 + yh * 2 + c
    places = itertools.product(range(2), range(4), range(4), range(2), range(2))
    return [(at(*p), at(*fn(*p))) for p in places]


WAYS = {
    "zP": way(lambda yl, z, x, yh, c: (yl, z + 1 - 2 * c, x, yh, c)),
    "zM": way(lambda yl, z, x, yh, c: (yl, z - 1 + 2 * c, x, yh, c)),
    "xP": way(lambda yl, z, x, yh, c: (yl, z, x + 1 - 2 * c, yh, c)),
    "xM": way(lambda yl, z, x, yh, c: (yl, z, x - 1 + 2 * c, yh, c)),
    "yl": way(lambda yl, z, x, yh, c: (1 - yl, z, x, yh, c)),
    "yh": way(lambda yl, z, x, yh, c: (yl, z, x, 1 - yh, c)),
    "co": way(lambda yl, z, x, yh, c: (yl, z, x, yh, 1 - c)),
}

STEPS = [
    ("t1", "yh", "t"), ("WP", "zP", "w"), ("tP", "xP", "t"), ("WM", "zM", "w"), ("tM", "xM", "t"), ("ct", "co", "t"),
    ("S1a", "yl", "Sa"), ("S1b", "yl", "Sb"),
    ("t1P", "xP", "t1"), ("t1M", "xM", "t1"), ("WD", "zP", "WP"),
    ("ct1", "co", "t1"), ("ctP", "co", "tP"), ("ctM", "co", "tM"), ("tD", "xP", "tP"),
    ("kA",),
    ("F1", "yl", "F"), ("F1P", "yl", "FP"), ("F1M", "yl", "FM"),
    ("S1aP", "zP", "S1a"), ("S1aM", "zM", "S1a"),
    ("kB",),
    ("S1bP", "zP", "S1b"), ("S1bM", "zM", "S1b"),
    ("kC",),
    ("kS",),
    ("t1Da", "xP", "t1Pa"), ("t1Db", "xP", "t1Pb"), ("ct1P", "co", "t1P"), ("ct1M", "co", "t1M"), ("F1D", "yl", "FD"),
    ("kD",),
    ("kF",),
    ("kE",),
    ("S1aD", "zP", "S1aP"),
    ("kH",),
    ("ctD", "co", "tD"), ("S1bD", "zP", "S1bP"),
    ("kJ",),
    ("kI",),
    ("ct1Da", "co", "t1Da"),
    ("kL",),
    ("ct1Db", "co", "t1Db"),
    ("kK",),
    ("kM",),
    ("kG",),
]
A = ["t", "tP", "tM", "t1", "ct", "ctP", "ctM", "ct1"]
B1 = ["t1P", "t1M", "ct1P", "ct1M"]
D0 = ["tD", "ctD"]
B2 = ["t1D", "ct1D"]

W0 = [(0, 0, [("w", 0, KB)]), (1, 0, [("WP", 0, KB)]), (2, 0, [("WM", 0, KB)])]
WD = [(3, 0, [("WD", 0, KB)])]
S1 = [(4, F, [("S1a", 0, HA), ("S1b", 0, HB)])]
W1 = [(4, 0, [("F1", 0, F)]), (5, 0, [("F1P", 0, F), ("S1aP", 0, HA)]), (6, F, [("S1aM", 0, HA)])]
W2 = [(5, F + HA, [("S1bP", 0, HB)]), (6, 0, [("F1M", 0, F)]), (6, F + HA, [("S1bM", 0, HB)])]
W3, W4, W5 = [(7, F, [("S1aD", 0, HA)])], [(7, 0, [("F1D", 0, F)])], [(7, F + HA, [("S1bD", 0, HB)])]

ALL = A + B1 + D0 + B2
B2_AT = ROWS * len(A + B1 + D0)


def piece_of(name, block):
    return name if name not in B2 else name + "b" if block in (5, 6) else name + "a"


KERNELS = {
    "kA": [(0, 768, W0)],
    "kB": [(0, 768, [(4, F, [("S1a", 0, HA)])])],
    "kC": [(0, 768, WD + [(4, F + HA, [("S1b", 0, HB)])])],
    "kD": [(768, 960, W0 + WD + S1)],
    "kE": [(0, 768, W1[::2])],
    "kF": [(960, 1152, W0 + WD + S1)],
    "kH": [(0, 768, W1[1:2]), (768, 1152, W1)],
    "kI": [(1152, 1344, W0 + WD + S1 + W1 + W2)],
    "kJ": [(0, 1152, W2)],
    "kL": [(0, 1344, W3)],
    "kK": [(1344, 1536, W0 + WD + S1 + W1[:1] + W3)],
    "kM": [(0, 1344, W4), (1344, 1536, W4)],
    "kG": [(0, 1344, W5), (1344, 1536, W5 + W1[1:] + W2)],
}
TILE = 384
VMEM, LAST_VMEM = 4, 6


def sum_of(parts):
    return functools.reduce(lambda a, b: a + b, parts)


def kernel(plan, *refs):
    row, col = lax.axis_index("row"), lax.axis_index("col")
    yl, z, x, yh, core = row // 4, row % 4, col // 4, col // 2 % 2, col % 2
    far = lambda name, c: 3 - 2 * c if "P" in name else 1 + 2 * c if "M" in name else 2 if "D" in name else 0
    block_at = [((yl ^ one) * 4 + (z + far(k, core)) % 4) * KB for one in range(2) for k in ("", "P", "M", "D")]
    block_in_piece = [block_at[b] - yl * (4 * KB) for b in range(4)]
    block_in_piece += [4 * KB, (far("P", core) - 1) // 2 * KB, (far("M", core) - 1) // 2 * KB, 5 * KB]
    n_t, n_w = len(plan["t"]), len(plan["w"])
    t_refs, w_refs, refs = refs[:n_t], refs[n_t : n_t + n_w], refs[n_t + n_w :]
    sums_ref, refs = (refs[0], refs[1:]) if plan["taken"] else (None, refs)
    out_ref, *rest = refs

    def product(r, e, piece):
        block, k, arrays = piece
        total = None
        for name, first, rows in arrays:
            at = (block_at[block] if r < B2_AT else block_in_piece[block]) + k
            cols = pl.ds(pl.multiple_of(at, 128), rows)
            lhs = [t_refs[plan["t"].index(piece_of(n, block))][:, cols] for n in ALL[r // ROWS : e // ROWS]]
            lhs = jnp.concatenate(lhs, axis=0)
            part = jnp.dot(lhs, w_refs[plan["w"].index(name)][first : first + rows], preferred_element_type=jnp.float32)
            total = part if total is None else total + part
            k += rows
        return total

    started = []
    for lo, hi, blocks in plan["groups"]:
        for r in range(lo, hi, TILE):
            e = min(hi, r + TILE)
            at = pl.ds(r, e - r)
            total = sum_of([product(r, e, block) for block in blocks])
            if blocks[0] not in W0:
                total = total + sums_ref[at]
            if not plan["last"]:
                out_ref[at] = total
                continue
            res, sem = rest
            res[at] = total.astype(jnp.bfloat16)
            for q in range(r // ROWS, e // ROWS):
                c = core ^ ("c" in ALL[q])
                place = (x + far(ALL[q], c)) % 4 * 4 + (yh ^ ("1" in ALL[q])) * 2 + c
                to = out_ref.at[pl.ds(pl.multiple_of(place * ROWS, 16), ROWS)]
                started.append(pltpu.make_async_copy(res.at[pl.ds(q * ROWS, ROWS)], to, sem.at[q]))
                started[-1].start()
    for copy in started:
        copy.wait()


def call(name, got, sums):
    groups, last = KERNELS[name], name == "kG"
    names, arrays = [], []
    for lo, hi, blocks in groups:
        for n in ALL[lo // ROWS : hi // ROWS]:
            names += [p for p in dict.fromkeys(piece_of(n, b[0]) for b in blocks) if p not in names]
    for _, _, blocks in groups:
        for block in blocks:
            arrays += [a for a, _, _ in block[2] if a not in arrays]
    plan = {"t": names, "w": arrays, "taken": sums is not None, "groups": groups, "last": last}
    flops = sum(2 * (hi - lo) * rows * N for lo, hi, blocks in groups for b in blocks for _, _, rows in b[2])
    vmem = pl.BlockSpec(memory_space=pltpu.VMEM)
    ins = [got[n] for n in names + arrays] + ([] if sums is None else [sums])
    ins = [pltpu.with_memory_space_constraint(v, pltpu.MemorySpace.VMEM) for v in ins]
    shape = (len(ALL) * ROWS, N)
    return pl.pallas_call(
        functools.partial(kernel, plan),
        out_shape=jax.ShapeDtypeStruct(shape, jnp.bfloat16) if last else pltpu.MemorySpace.VMEM(shape, jnp.float32),
        in_specs=[vmem] * len(ins),
        out_specs=pl.BlockSpec(memory_space=pltpu.HBM) if last else vmem,
        input_output_aliases={} if last or sums is None else {len(ins) - 1: 0},
        scratch_shapes=[pltpu.VMEM(shape, jnp.bfloat16), pltpu.SemaphoreType.DMA((len(ALL),))] if last else [],
        compiler_params=pltpu.CompilerParams(vmem_limit_bytes=(LAST_VMEM if last else VMEM) * 2**20),
        cost_estimate=pl.CostEstimate(flops=flops, bytes_accessed=flops // 1000, transcendentals=0),
    )(*ins)


def two_pieces(whole, a, b):
    row = lax.axis_index("row")
    yl, z = row // 4, row % 4
    columns = lambda block, n: whole[:, pl.ds(pl.multiple_of(block * KB, KB), n * KB)]
    a[:, : 4 * KB] = columns(yl * 4, 4)
    a[:, 4 * KB : 5 * KB] = columns((1 - yl) * 4 + z, 1)
    a[:, 5 * KB :] = columns((1 - yl) * 4 + (z + 2) % 4, 1)
    b[:, :KB] = columns((1 - yl) * 4 + (z + 1) % 4, 1)
    b[:, KB:] = columns((1 - yl) * 4 + (z + 3) % 4, 1)


def first_rows(whole, out):
    out[...] = whole[:F]


def cut(whole, body, shapes):
    vmem = pl.BlockSpec(memory_space=pltpu.VMEM)
    return pl.pallas_call(
        body,
        out_shape=[pltpu.MemorySpace.VMEM(shape, jnp.bfloat16) for shape in shapes],
        in_specs=[vmem],
        out_specs=[vmem] * len(shapes),
        compiler_params=pltpu.CompilerParams(vmem_limit_bytes=VMEM * 2**20),
        name="kS",
    )(pltpu.with_memory_space_constraint(whole, pltpu.MemorySpace.VMEM))


def on_device(tokens, up_weight):
    got = {"t": tokens, "w": up_weight, "F": up_weight[:F], "Sa": up_weight[F : F + HA], "Sb": up_weight[F + HA :]}
    sums = None
    for step in STEPS:
        if len(step) == 3 and step[2] in ("FP", "FM", "FD"):
            (got[step[2]],) = cut(got["W" + step[2][1]], first_rows, [(F, N)])
        if len(step) == 3:
            got[step[0]] = lax.ppermute(got[step[2]], ("row", "col"), WAYS[step[1]])
        elif step == ("kS",):
            got["t1Pa"], got["t1Pb"] = cut(got["t1P"], two_pieces, [(ROWS, 6 * KB), (ROWS, 2 * KB)])
        else:
            sums = call(step[0], got, sums)
    return sums


def solution(mesh):
    return jax.shard_map(
        on_device, mesh=mesh, in_specs=(P(("row", "col"), None), P("row", "col")), out_specs=P("row", "col"), check_vma=False
    )
```

```python
import functools
import itertools

import jax
import jax.numpy as jnp
from jax import lax
from jax.experimental import pallas as pl
from jax.experimental.pallas import tpu as pltpu
from jax.sharding import PartitionSpec as P

N = 896
KB = 1024
ROWS = 96


F = 256
HA, HB = 512, 256


def way(fn):
    at = lambda yl, z, x, yh, c: (yl * 4 + z % 4) * 16 + x % 4 * 4 + yh * 2 + c
    places = itertools.product(range(2), range(4), range(4), range(2), range(2))
    return [(at(*p), at(*fn(*p))) for p in places]


WAYS = {
    "zP": way(lambda yl, z, x, yh, c: (yl, z + 1 - 2 * c, x, yh, c)),
    "zM": way(lambda yl, z, x, yh, c: (yl, z - 1 + 2 * c, x, yh, c)),
    "xP": way(lambda yl, z, x, yh, c: (yl, z, x + 1 - 2 * c, yh, c)),
    "xM": way(lambda yl, z, x, yh, c: (yl, z, x - 1 + 2 * c, yh, c)),
    "yl": way(lambda yl, z, x, yh, c: (1 - yl, z, x, yh, c)),
    "yh": way(lambda yl, z, x, yh, c: (yl, z, x, 1 - yh, c)),
    "co": way(lambda yl, z, x, yh, c: (yl, z, x, yh, 1 - c)),
}

STEPS = [
    ("t1", "yh", "t"), ("WP", "zP", "w"), ("tP", "xP", "t"), ("WM", "zM", "w"), ("tM", "xM", "t"), ("ct", "co", "t"),
    ("S1a", "yl", "Sa"), ("S1b", "yl", "Sb"),
    ("t1P", "xP", "t1"), ("t1M", "xM", "t1"), ("WD", "zP", "WP"),
    ("ct1", "co", "t1"), ("ctP", "co", "tP"), ("ctM", "co", "tM"), ("tD", "xP", "tP"),
    ("kA",),
    ("F1", "yl", "F"), ("F1P", "yl", "FP"), ("F1M", "yl", "FM"),
    ("S1aP", "zP", "S1a"), ("S1aM", "zM", "S1a"),
    ("kB",),
    ("S1bP", "zP", "S1b"), ("S1bM", "zM", "S1b"),
    ("kC",),
    ("kS",),
    ("t1Da", "xP", "t1Pa"), ("t1Db", "xP", "t1Pb"), ("ct1P", "co", "t1P"), ("ct1M", "co", "t1M"), ("F1D", "yl", "FD"),
    ("kD",),
    ("kF",),
    ("kE",),
    ("S1aD", "zP", "S1aP"),
    ("kH",),
    ("ctD", "co", "tD"), ("S1bD", "zP", "S1bP"),
    ("kJ",),
    ("ct1Da", "co", "t1Da"),
    ("kI",),
    ("kK",),
    ("kL",),
    ("ct1Db", "co", "t1Db"),
    ("kM",),
    ("kG",),
]
A = ["t", "tP", "tM", "t1", "ct", "ctP", "ctM", "ct1"]
B1 = ["t1P", "t1M", "ct1P", "ct1M"]
D0 = ["tD", "ctD"]
B2 = ["t1D", "ct1D"]

W0 = [(0, 0, [("w", 0, KB)]), (1, 0, [("WP", 0, KB)]), (2, 0, [("WM", 0, KB)])]
WD = [(3, 0, [("WD", 0, KB)])]
S1 = [(4, F, [("S1a", 0, HA), ("S1b", 0, HB)])]
W1 = [(4, 0, [("F1", 0, F)]), (5, 0, [("F1P", 0, F), ("S1aP", 0, HA)]), (6, F, [("S1aM", 0, HA)])]
W2 = [(5, F + HA, [("S1bP", 0, HB)]), (6, 0, [("F1M", 0, F)]), (6, F + HA, [("S1bM", 0, HB)])]
W3, W4, W5 = [(7, F, [("S1aD", 0, HA)])], [(7, 0, [("F1D", 0, F)])], [(7, F + HA, [("S1bD", 0, HB)])]

ALL = A + B1 + D0 + B2
B2_AT = ROWS * len(A + B1 + D0)


def piece_of(name, block):
    return name if name not in B2 else name + "b" if block > 4 else name + "a"


KERNELS = {
    "kA": [(0, 768, W0)],
    "kB": [(0, 768, [(4, F, [("S1a", 0, HA)])])],
    "kC": [(0, 768, WD + [(4, F + HA, [("S1b", 0, HB)])])],
    "kD": [(768, 960, W0 + WD + S1)],
    "kE": [(0, 768, W1[::2])],
    "kF": [(960, 1152, W0 + WD + S1)],
    "kH": [(0, 768, W1[1:2]), (768, 1152, W1)],
    "kI": [(1152, 1344, W0 + WD + S1 + W1 + W2)],
    "kJ": [(0, 1152, W2)],
    "kL": [(0, 1344, W3)],
    "kK": [(1344, 1536, W0 + WD + S1 + W1[:1])],
    "kM": [(0, 1344, W4)],
    "kG": [(0, 1344, W5), (1344, 1536, W1[1:] + W2 + W3 + W4 + W5)],
}
TILE = 384
VMEM, LAST_VMEM = 4, 6


def sum_of(parts):
    return functools.reduce(lambda a, b: a + b, parts)


def kernel(plan, *refs):
    row, col = lax.axis_index("row"), lax.axis_index("col")
    yl, z, x, yh, core = row // 4, row % 4, col // 4, col // 2 % 2, col % 2
    far = lambda name, c: 3 - 2 * c if "P" in name else 1 + 2 * c if "M" in name else 2 if "D" in name else 0
    block_at = [((yl ^ one) * 4 + (z + far(k, core)) % 4) * KB for one in range(2) for k in ("", "P", "M", "D")]
    block_in_piece = [block_at[b] - yl * (4 * KB) for b in range(4)]
    block_in_piece += [4 * KB, (far("P", core) - 1) // 2 * KB, (far("M", core) - 1) // 2 * KB, 2 * KB]
    n_t, n_w = len(plan["t"]), len(plan["w"])
    t_refs, w_refs, refs = refs[:n_t], refs[n_t : n_t + n_w], refs[n_t + n_w :]
    sums_ref, refs = (refs[0], refs[1:]) if plan["taken"] else (None, refs)
    out_ref, *rest = refs

    def product(r, e, piece):
        block, k, arrays = piece
        total = None
        for name, first, rows in arrays:
            at = (block_at[block] if r < B2_AT else block_in_piece[block]) + k
            cols = pl.ds(pl.multiple_of(at, 128), rows)
            lhs = [t_refs[plan["t"].index(piece_of(n, block))][:, cols] for n in ALL[r // ROWS : e // ROWS]]
            lhs = jnp.concatenate(lhs, axis=0)
            part = jnp.dot(lhs, w_refs[plan["w"].index(name)][first : first + rows], preferred_element_type=jnp.float32)
            total = part if total is None else total + part
            k += rows
        return total

    started = []
    for lo, hi, blocks in plan["groups"]:
        for r in range(lo, hi, TILE):
            e = min(hi, r + TILE)
            at = pl.ds(r, e - r)
            total = sum_of([product(r, e, block) for block in blocks])
            if blocks[0] not in W0:
                total = total + sums_ref[at]
            if not plan["last"]:
                out_ref[at] = total
                continue
            res, sem = rest
            res[at] = total.astype(jnp.bfloat16)
            for q in range(r // ROWS, e // ROWS):
                c = core ^ ("c" in ALL[q])
                place = (x + far(ALL[q], c)) % 4 * 4 + (yh ^ ("1" in ALL[q])) * 2 + c
                to = out_ref.at[pl.ds(pl.multiple_of(place * ROWS, 16), ROWS)]
                started.append(pltpu.make_async_copy(res.at[pl.ds(q * ROWS, ROWS)], to, sem.at[q]))
                started[-1].start()
    for copy in started:
        copy.wait()


def call(name, got, sums):
    groups, last = KERNELS[name], name == "kG"
    names, arrays = [], []
    for lo, hi, blocks in groups:
        for n in ALL[lo // ROWS : hi // ROWS]:
            names += [p for p in dict.fromkeys(piece_of(n, b[0]) for b in blocks) if p not in names]
    for _, _, blocks in groups:
        for block in blocks:
            arrays += [a for a, _, _ in block[2] if a not in arrays]
    plan = {"t": names, "w": arrays, "taken": sums is not None, "groups": groups, "last": last}
    flops = sum(2 * (hi - lo) * rows * N for lo, hi, blocks in groups for b in blocks for _, _, rows in b[2])
    vmem = pl.BlockSpec(memory_space=pltpu.VMEM)
    ins = [got[n] for n in names + arrays] + ([] if sums is None else [sums])
    ins = [pltpu.with_memory_space_constraint(v, pltpu.MemorySpace.VMEM) for v in ins]
    shape = (len(ALL) * ROWS, N)
    return pl.pallas_call(
        functools.partial(kernel, plan),
        out_shape=jax.ShapeDtypeStruct(shape, jnp.bfloat16) if last else pltpu.MemorySpace.VMEM(shape, jnp.float32),
        in_specs=[vmem] * len(ins),
        out_specs=pl.BlockSpec(memory_space=pltpu.HBM) if last else vmem,
        input_output_aliases={} if last or sums is None else {len(ins) - 1: 0},
        scratch_shapes=[pltpu.VMEM(shape, jnp.bfloat16), pltpu.SemaphoreType.DMA((len(ALL),))] if last else [],
        compiler_params=pltpu.CompilerParams(vmem_limit_bytes=(LAST_VMEM if last else VMEM) * 2**20),
        cost_estimate=pl.CostEstimate(flops=flops, bytes_accessed=flops // 1000, transcendentals=0),
    )(*ins)


def two_pieces(whole, a, b):
    row = lax.axis_index("row")
    yl, z = row // 4, row % 4
    columns = lambda block, n: whole[:, pl.ds(pl.multiple_of(block * KB, KB), n * KB)]
    a[:, : 4 * KB] = columns(yl * 4, 4)
    a[:, 4 * KB :] = columns((1 - yl) * 4 + z, 1)
    b[:, :KB] = columns((1 - yl) * 4 + (z + 1) % 4, 1)
    b[:, KB : 2 * KB] = columns((1 - yl) * 4 + (z + 3) % 4, 1)
    b[:, 2 * KB :] = columns((1 - yl) * 4 + (z + 2) % 4, 1)


def first_rows(whole, out):
    out[...] = whole[:F]


def cut(whole, body, shapes):
    vmem = pl.BlockSpec(memory_space=pltpu.VMEM)
    return pl.pallas_call(
        body,
        out_shape=[pltpu.MemorySpace.VMEM(shape, jnp.bfloat16) for shape in shapes],
        in_specs=[vmem],
        out_specs=[vmem] * len(shapes),
        compiler_params=pltpu.CompilerParams(vmem_limit_bytes=VMEM * 2**20),
        name="kS",
    )(pltpu.with_memory_space_constraint(whole, pltpu.MemorySpace.VMEM))


def on_device(tokens, up_weight):
    got = {"t": tokens, "w": up_weight, "F": up_weight[:F], "Sa": up_weight[F : F + HA], "Sb": up_weight[F + HA :]}
    sums = None
    for step in STEPS:
        if len(step) == 3 and step[2] in ("FP", "FM", "FD"):
            (got[step[2]],) = cut(got["W" + step[2][1]], first_rows, [(F, N)])
        if len(step) == 3:
            got[step[0]] = lax.ppermute(got[step[2]], ("row", "col"), WAYS[step[1]])
        elif step == ("kS",):
            got["t1Pa"], got["t1Pb"] = cut(got["t1P"], two_pieces, [(ROWS, 5 * KB), (ROWS, 3 * KB)])
        else:
            sums = call(step[0], got, sums)
    return sums


def solution(mesh):
    return jax.shard_map(
        on_device, mesh=mesh, in_specs=(P(("row", "col"), None), P("row", "col")), out_specs=P("row", "col"), check_vma=False
    )
```
